128 devices in a mesh: group: 2 (over core), ctx: 32 (over y_hi, z, x), mp: 2 (over y_lo).
Axes of the slice: x: 4, y: 4 (y_hi: 2, y_lo: 2; y = y_hi * 2 + y_lo), z: 4, core: 2. Of those that a mesh axis runs over, the one named last changes fastest.
Arguments:
- token_ids: int32 [2, 4096], P('group', 'ctx'), may hold values from 0 to 127
- span_offset: int32 [1], replicated, may hold values from 0 to 12287
- shard_lengths: int32 [32], P('ctx'), may hold values from 1 to 384
- embed_table: bfloat16 [128, 2560], P(None, 'mp'), may hold values from -6 to 6
- norm_gain: bfloat16 [2560], P('mp'), may hold values from 0.25 to 1.75
- query_weight: bfloat16 [2560, 2560], P('mp'), may hold values from -0.25 to 0.25
- key_weight: bfloat16 [2560, 2560], P('mp'), may hold values from -0.25 to 0.25
- value_weight: bfloat16 [2560, 2560], P('mp'), may hold values from -0.125 to 0.125
- cache_keys: bfloat16 [12288, 2560], P('ctx', 'mp'), may hold values from -440 to 440
- cache_values: bfloat16 [12288, 2560], P('ctx', 'mp'), may hold values from -6 to 6
Outputs:
- attended: bfloat16 [2, 4096, 2560], P('group', 'ctx', 'mp')
The draws below stay inside these ranges and needn't reach their ends.
All inputs are finite; a program needn't handle non-finite values.
Results may differ from the reference program's by a relative error of at most 0.012.
The reference program's roundings to bfloat16 on the way (of `normal_rows`) count: a program that leaves them out, or rounds other values in their place, can miss the bound.
Values may be sent and summed in bfloat16 or wider, within the bound.
No kernel may reach another device: no remote copies, remote signals or barrier semaphores. Data moves between devices by JAX's collectives and lax.ppermute only.
A program may use at most 256 MiB of HBM per device.

```python
import math
import jax
import jax.numpy as jnp
from jax import lax

D = 2560
HEADS = 32
HD = 80
VOCAB = 128
PROT = 256
STEPS = 4
ROWS_DEV = 128
CACHE_DEV = 384
SPAN = 4096
CONTEXT = 12288
N_CTX = 32


def draw_cache_keys(key, part):
    normal_part = jax.random.normal(key, (CONTEXT, D), jnp.float32) * 2.0
    result = jnp.clip(normal_part, -12.0, 12.0)
    return result.astype(jnp.bfloat16)


def plant(values, own_key, least, high):
    dims = values.shape
    index_at = [jax.random.randint(jax.random.fold_in(own_key, axis), (), 0, dims[axis]) for axis in range(len(dims))]
    values = values.at[tuple(index_at)].set(least)
    longest = dims.index(max(dims))
    index_at[longest] = (index_at[longest] + 1) % dims[longest]
    return values.at[tuple(index_at)].set(high)


def levels(rng, extent, shards, least, top_value):
    gain, own = 1.0, jax.random.fold_in(rng, 6)
    for axis_at, shards_of in shards:
        draws = jnp.exp(jax.random.uniform(jax.random.fold_in(own, axis_at), (shards_of,), jnp.float32, least / len(shards), top_value / len(shards)))
        gain = gain * jnp.repeat(draws, extent[axis_at] // shards_of).reshape([-1 if axis == axis_at else 1 for axis in range(len(extent))])
    return gain


def normal_values(stream_key, extent, width, reach, shards=(), held_as=jnp.bfloat16):
    level = levels(stream_key, extent, shards, -0.22, 0.18) if shards else 1.0
    drawn = jax.random.normal(stream_key, extent, jnp.float32) * width * level
    return jnp.minimum(jnp.maximum(drawn, -reach), reach).astype(held_as)


def setup_inputs(seed: int = 0) -> dict:
    key_list = jax.random.split(jax.random.key(seed), 11)
    return {
        "token_ids": plant(jax.random.randint(key_list[0], (2, SPAN), 0, VOCAB), jax.random.fold_in(key_list[0], 1), 0, VOCAB - 1).astype(jnp.int32),
        "span_offset": jax.random.randint(key_list[1], (1,), 0, CONTEXT).astype(jnp.int32),
        "shard_lengths": plant(jax.random.randint(key_list[2], (N_CTX,), 1, CACHE_DEV + 1), jax.random.fold_in(key_list[2], 1), 1, CACHE_DEV).astype(jnp.int32),
        "embed_table": normal_values(key_list[3], (VOCAB, D), 1.0, 6.0, ((1, 2),)),
        "norm_gain": jnp.clip(1.0 + 0.15 * jax.random.normal(key_list[4], (D,), jnp.float32), 0.25, 1.75).astype(jnp.bfloat16),
        "query_weight": normal_values(key_list[5], (D, D), (D // 4) ** -0.5, 0.25, ((0, 2),)),
        "key_weight": normal_values(key_list[6], (D, D), (D // 4) ** -0.5, 0.25, ((0, 2),)),
        "value_weight": normal_values(key_list[7], (D, D), D ** -0.5, 0.125, ((0, 2),)),
        "cache_keys": draw_cache_keys(jax.random.fold_in(key_list[10], 71), 0),
        "cache_values": normal_values(key_list[9], (CONTEXT, D), 1.0, 6.0, ((0, 32), (1, 2))),
    }


def rotate(values_in, positions):
    row_count = values_in.shape[0]
    head_count = values_in.shape[1] // HD
    quarter = HD // 4
    column = (positions % PROT).astype(jnp.float32)
    homolog = (positions // PROT).astype(jnp.float32)
    frequency = 10000.0 ** (-jnp.arange(quarter, dtype=jnp.float32) / quarter)
    angles = jnp.stack([column[:, None] * frequency, homolog[:, None] * frequency], 1)
    cosine = jnp.cos(angles)[:, None, :, None, :]
    sine_table = jnp.sin(angles)[:, None, :, None, :]
    pieces = values_in.reshape(row_count, head_count, 2, 2, quarter)
    partner = jnp.stack([-pieces[:, :, :, 1], pieces[:, :, :, 0]], 3)
    return (pieces * cosine + partner * sine_table).reshape(row_count, head_count * HD)

def normed(embedded, gain_vector):
    mean_square = lax.optimization_barrier(jnp.mean(embedded * embedded, -1, keepdims=True))
    return (embedded * lax.rsqrt(mean_square + 1e-05) * gain_vector.astype(jnp.float32)).astype(jnp.bfloat16)

def reference(token_ids, span_offset, shard_lengths, embed_table, norm_gain, query_weight, key_weight, value_weight, cache_keys, cache_values):
    score_scale = 1.0 / math.sqrt(HD)
    embedded = embed_table[token_ids].astype(jnp.float32).reshape(2 * SPAN, D)
    normal_rows = normed(embedded, norm_gain)
    query_full = jnp.dot(normal_rows, query_weight, preferred_element_type=jnp.float32)
    key_full = jnp.dot(normal_rows, key_weight, preferred_element_type=jnp.float32)
    value_full = jnp.dot(normal_rows, value_weight, preferred_element_type=jnp.float32)
    row_iota = jnp.arange(SPAN, dtype=jnp.int32)
    offset_value = span_offset[0]
    positions = jnp.concatenate([offset_value + row_iota, offset_value + SPAN + row_iota % STEPS])
    queries = rotate(query_full, positions).astype(jnp.bfloat16).reshape(2, SPAN, HEADS, HD)
    new_keys = rotate(key_full, positions).astype(jnp.bfloat16).reshape(2, SPAN, HEADS, HD)
    new_values = value_full.astype(jnp.bfloat16).reshape(2, SPAN, HEADS, HD)
    cache_k = cache_keys.reshape(CONTEXT, HEADS, HD)
    cache_v = cache_values.reshape(CONTEXT, HEADS, HD)
    key_slots = CACHE_DEV + ROWS_DEV
    slot = jnp.arange(key_slots, dtype=jnp.int32)
    results = []
    for group_index in range(2):
        query_group = queries[group_index].astype(jnp.float32)

        def shard_step(carry, shard):
            big_max, big_sum, big_acc = carry
            start_cache = (shard * CACHE_DEV).astype(jnp.int32)
            start_span = (shard * ROWS_DEV).astype(jnp.int32)
            keys_here = jnp.concatenate([lax.dynamic_slice_in_dim(cache_k, start_cache, CACHE_DEV, 0), lax.dynamic_slice_in_dim(new_keys[0], start_span, ROWS_DEV, 0)], 0)
            values_here = jnp.concatenate([lax.dynamic_slice_in_dim(cache_v, start_cache, CACHE_DEV, 0), lax.dynamic_slice_in_dim(new_values[0], start_span, ROWS_DEV, 0)], 0)
            scores = jnp.einsum('qhd,khd->hqk', query_group, keys_here.astype(jnp.float32)) * score_scale
            cache_live = (slot < CACHE_DEV) & (slot < shard_lengths[shard])
            span_index = start_span + slot - CACHE_DEV
            span_seen = (slot >= CACHE_DEV)[None, :] & ((group_index == 1) | (span_index[None, :] <= row_iota[:, None]))
            visible = (cache_live[None, :] | span_seen)[None]
            shard_max = lax.optimization_barrier(jnp.max(jnp.where(visible, scores, -1e+30), -1))
            weights = jnp.where(visible, jnp.exp(scores - shard_max[..., None]), 0.0)
            shard_sum = lax.optimization_barrier(jnp.sum(weights, -1))
            shard_acc = jnp.einsum('hqk,khd->hqd', weights.astype(jnp.bfloat16).astype(jnp.float32), values_here.astype(jnp.float32))
            new_max = jnp.maximum(big_max, shard_max)
            keep_old = jnp.exp(big_max - new_max)
            keep_new = jnp.exp(shard_max - new_max)
            return ((new_max, big_sum * keep_old + shard_sum * keep_new, big_acc * keep_old[..., None] + shard_acc * keep_new[..., None]), None)
        start_state = (jnp.full((HEADS, SPAN), -1e+30, jnp.float32), jnp.zeros((HEADS, SPAN), jnp.float32), jnp.zeros((HEADS, SPAN, HD), jnp.float32))
        (whole_max, whole_sum, whole_acc), unused = lax.scan(shard_step, start_state, jnp.arange(N_CTX, dtype=jnp.int32))
        cands = SPAN // STEPS
        own_q = query_group.reshape(cands, STEPS, HEADS, HD)
        own_k = new_keys[group_index].astype(jnp.float32).reshape(cands, STEPS, HEADS, HD)
        own_v = new_values[group_index].astype(jnp.float32).reshape(cands, STEPS, HEADS, HD)
        own_scores = jnp.einsum('ashd,athd->ahst', own_q, own_k) * score_scale
        step_iota = jnp.arange(STEPS, dtype=jnp.int32)
        own_visible = (step_iota[None, :] <= step_iota[:, None]) & (group_index == 1)
        own_max = lax.optimization_barrier(jnp.max(jnp.where(own_visible, own_scores, -1e+30), -1))
        own_max_rows = own_max.transpose(1, 0, 2).reshape(HEADS, SPAN)
        final_max = jnp.maximum(whole_max, own_max_rows)
        keep_old = jnp.exp(whole_max - final_max)
        final_cand = final_max.reshape(HEADS, cands, STEPS).transpose(1, 0, 2)
        own_weights = jnp.where(own_visible, jnp.exp(own_scores - final_cand[..., None]), 0.0)
        own_sum = lax.optimization_barrier(jnp.sum(own_weights, -1)).transpose(1, 0, 2).reshape(HEADS, SPAN)
        own_acc = jnp.einsum('ahst,athd->hasd', own_weights.astype(jnp.bfloat16).astype(jnp.float32), own_v).reshape(HEADS, SPAN, HD)
        numer = whole_acc * keep_old[..., None] + own_acc
        denom = whole_sum * keep_old + own_sum
        output = (numer / denom[..., None]).transpose(1, 0, 2).reshape(SPAN, D)
        results.append(output.astype(jnp.bfloat16))
    return jnp.stack(results, 0)
```

```python
import math

import jax
import jax.numpy as jnp
from jax import lax
from jax.experimental import pallas as pl
from jax.experimental.pallas import tpu as pltpu
from jax.sharding import Mesh
from jax.sharding import PartitionSpec as P

D = 2560
HALF = 1280
HD = 80
PROT = 256
STEPS = 4
VOCAB = 128
PLANE = 16
N_CTX = 32
ROWS = 128
CACHE = 384
TILE = 256
SLOTS = 10
SENT = 6
GS = 2
KB = 1024
KB_NEW = 512
SCALE2 = math.log2(math.e) / math.sqrt(HD)
LOW = -1e30
DEAD = -2e30
F32 = jnp.float32
BF16 = jnp.bfloat16
TILES = ((0, 1, 2, 3, 10, 11, 12, 13, 14, 15), (4, 5, 6, 7, 8, 9, 16, 17, 0, 0))


def vm():
    return pl.BlockSpec(memory_space=pltpu.MemorySpace.VMEM)


def sm():
    return pl.BlockSpec(memory_space=pltpu.MemorySpace.SMEM)


def anyspace():
    return pl.BlockSpec(memory_space=pl.ANY)


def params():
    return pltpu.CompilerParams(vmem_limit_bytes=56 << 20)


def split3(x):
    high = x.astype(BF16)
    rest = x - high.astype(F32)
    mid = rest.astype(BF16)
    low = (rest - mid.astype(F32)).astype(BF16)
    return high, mid, low


def first_row(shape, value):
    return jnp.where(lax.broadcasted_iota(jnp.int32, shape, 0) == 0, value, 0.0)


def turn_kernel(where_ref, keys_ref, values_ref, out_ref, buf, sem):
    @pl.when(where_ref[0] == 0)
    def _():
        pltpu.make_async_copy(keys_ref, buf, sem).start()

    @pl.when(where_ref[0] != 0)
    def _():
        pltpu.make_async_copy(values_ref, buf, sem).start()

    pltpu.make_async_copy(keys_ref, buf, sem).wait()
    for block in range(HALF // 128):
        out_ref[block * 128 : block * 128 + 128, :] = buf[:, block * 128 : block * 128 + 128].T


def turn(where, keys, values):
    return pl.pallas_call(
        turn_kernel,
        out_shape=jax.ShapeDtypeStruct((HALF, CACHE), BF16),
        in_specs=[sm(), anyspace(), anyspace()],
        out_specs=vm(),
        scratch_shapes=[pltpu.VMEM((CACHE, HALF), BF16), pltpu.SemaphoreType.DMA(())],
        compiler_params=params(),
        name="turn",
    )(where, keys, values)


def table_kernel(where_ref, embed_ref, gain_ref, square_ref, wq, wk, wv, own_ref, other_ref, buf, turned, sems):
    mp = where_ref[2]
    head = where_ref[3]
    base = jnp.minimum((head * HD) // 128 * 128, 1024)
    inside = pl.multiple_of(head * HD - base, 16)
    halves = (mp, 1 - mp)
    for half in range(2):
        at = pl.multiple_of(halves[half] * HALF + base, 128)
        for which, weight in enumerate((wq, wk, wv)):
            pltpu.make_async_copy(
                weight.at[:, pl.ds(at, 256)], buf.at[half * 3 + which], sems.at[half * 3 + which]
            ).start()
    mean = square_ref[...] / D
    normal = (
        embed_ref[...].astype(F32) * lax.rsqrt(mean + 1e-05) * gain_ref[...].astype(F32)
    ).astype(BF16)
    for half in (1, 0):
        for which in range(3):
            pltpu.make_async_copy(
                wq.at[:, pl.ds(0, 256)], buf.at[half * 3 + which], sems.at[half * 3 + which]
            ).wait()
            turned[...] = jnp.dot(normal, buf[half * 3 + which], preferred_element_type=F32).T
            out = own_ref if half == 0 else other_ref
            out[which * HD : which * HD + HD, :] = turned[pl.ds(inside, HD), :]


def table(where, embed, gain, square, wq, wk, wv):
    return pl.pallas_call(
        table_kernel,
        out_shape=[jax.ShapeDtypeStruct((3 * HD, VOCAB), F32)] * 2,
        in_specs=[sm(), vm(), vm(), vm(), anyspace(), anyspace(), anyspace()],
        out_specs=[vm(), vm()],
        scratch_shapes=[
            pltpu.VMEM((6, HALF, 256), BF16),
            pltpu.VMEM((256, VOCAB), F32),
            pltpu.SemaphoreType.DMA((6,)),
        ],
        compiler_params=params(),
        name="table",
    )(where, embed, gain, square, wq, wk, wv)


def flash_step(queries, keys, values, state_max, state_acc, limit=None, key_index=None):
    scores = jnp.dot(keys, queries, preferred_element_type=F32)
    if limit is not None:
        scores = jnp.where(key_index <= limit, scores, DEAD)
    new_max = jnp.maximum(state_max, jnp.max(scores, 0, keepdims=True))
    weights = jnp.exp2(scores - new_max).astype(BF16)
    acc = state_acc * jnp.exp2(state_max - new_max) + jnp.dot(
        values, weights, preferred_element_type=F32
    )
    return new_max, acc


def fresh_kernel(
    where_ref,
    own_ref,
    recv_ref,
    ids_ref,
    dec_ref,
    cos_ref,
    sin_ref,
    query_ref,
    max_ref,
    acc_ref,
    own_out,
    keys,
    values,
    wide,
):
    group = where_ref[0]
    plane = where_ref[1]
    quarter = HD // 4
    tables = own_ref[...] + recv_ref[...]
    row = lax.broadcasted_iota(jnp.int32, (HD, VOCAB), 0)
    upper = (row // quarter) % 2 == 0

    def stacked(part):
        partner = jnp.where(
            upper, -pltpu.roll(part, HD - quarter, 0), pltpu.roll(part, quarter, 0)
        )
        pieces = []
        for item in (part, partner):
            high = item.astype(BF16)
            pieces += [high, (item - high.astype(F32)).astype(BF16)]
        return jnp.concatenate(pieces, 0)

    query_table = stacked(tables[0:HD])
    key_table = stacked(tables[HD : 2 * HD])
    value_table = tables[2 * HD :].astype(BF16)
    tail_keys = jnp.zeros((16, TILE), BF16)
    ones_row = first_row((16, TILE), 1.0).astype(BF16)

    def chosen(tile):
        return (
            lax.broadcasted_iota(jnp.int32, (VOCAB, TILE), 0) == ids_ref[tile]
        ).astype(BF16)

    def turned_by(one_hot, stack, tile):
        raw = jnp.dot(stack, one_hot, preferred_element_type=F32)
        plain = raw[0:HD] + raw[HD : 2 * HD]
        partner = raw[2 * HD : 3 * HD] + raw[3 * HD :]
        return (plain * cos_ref[tile] + partner * sin_ref[tile]).astype(BF16)

    def tile_of(slot):
        return where_ref[4 + slot]

    def one_query(slot, carry):
        tile = tile_of(slot)
        rotated = turned_by(chosen(tile), query_table, tile)
        query_ref[slot] = jnp.concatenate([*split3(rotated.astype(F32) * SCALE2), ones_row], 0)
        return carry

    lax.fori_loop(0, SLOTS, one_query, 0, unroll=2)

    def one_key(block, carry):
        tile = 2 * block + plane
        one_hot = chosen(tile)
        rotated = turned_by(one_hot, key_table, tile)
        keys[block] = jnp.concatenate([rotated, rotated, rotated, tail_keys], 0).T
        picked = jnp.dot(value_table, one_hot, preferred_element_type=F32).astype(BF16)
        values[block] = jnp.concatenate([picked, ones_row], 0)
        return carry

    lax.fori_loop(0, 8, one_key, 0, unroll=2)

    for first in range(0, SLOTS, GS):
        last_tile = tile_of(first + GS - 1)
        most = jnp.where(last_tile >= PLANE, 8, (last_tile - plane) // 2 + 1)
        most = jnp.where((first >= 8) & (group == 1), 0, most)
        chunks = (most + 1) // 2
        for slot in range(first, first + GS):
            max_ref[slot] = jnp.full((1, TILE), LOW, F32)
            acc_ref[slot] = jnp.zeros((96, TILE), F32)

        def chunk(step, carry, first=first):
            key_part = jnp.concatenate([keys[2 * step], keys[2 * step + 1]], 0)
            value_part = jnp.concatenate([values[2 * step], values[2 * step + 1]], 1)
            row_at = lax.broadcasted_iota(jnp.int32, (KB_NEW, TILE), 0)
            key_index = row_at + jnp.where(row_at >= TILE, TILE, 0) + (4 * step + plane) * TILE
            lane = lax.broadcasted_iota(jnp.int32, (1, TILE), 1)
            for slot in range(first, first + GS):
                tile = tile_of(slot)
                limit = jnp.where(tile >= PLANE, 1 << 20, tile * TILE) + lane
                max_ref[slot], acc_ref[slot] = flash_step(
                    query_ref[slot],
                    key_part,
                    value_part,
                    max_ref[slot],
                    acc_ref[slot],
                    limit,
                    key_index,
                )
            return carry

        lax.fori_loop(0, chunks, chunk, 0)

    @pl.when(group == 1)
    def _():
        for part in range(2):
            lanes = slice(part * TILE, part * TILE + TILE)
            one_hot = chosen(16 + part)
            wide[0 : 3 * HD, lanes] = query_ref[SENT + part, 0 : 3 * HD, :]
            wide[3 * HD : 4 * HD, lanes] = turned_by(one_hot, key_table, 16 + part)
            wide[4 * HD : 5 * HD, lanes] = jnp.dot(
                value_table, one_hot, preferred_element_type=F32
            ).astype(BF16)
        key_at = lax.broadcasted_iota(jnp.int32, (ROWS, ROWS), 0)
        query_at = lax.broadcasted_iota(jnp.int32, (ROWS, ROWS), 1)
        seen = (key_at // STEPS == query_at // STEPS) & (key_at <= query_at)
        ones_tail = first_row((16, ROWS), 1.0).astype(BF16)
        zero_tail = jnp.zeros((16, ROWS), BF16)

        def one_block(item, carry):
            one_hot = decode_choice(dec_ref[plane * PLANE + item])
            picked = jnp.dot(wide[...], one_hot, preferred_element_type=F32).astype(BF16)
            queries = jnp.concatenate([picked[0 : 3 * HD], ones_tail], 0)
            own_keys = picked[3 * HD : 4 * HD]
            own_keys = jnp.concatenate([own_keys, own_keys, own_keys, zero_tail], 0).T
            scores = jnp.dot(own_keys, queries, preferred_element_type=F32)
            scores = jnp.where(seen, scores, DEAD)
            top = jnp.max(scores, 0, keepdims=True)
            weights = jnp.exp2(scores - top).astype(BF16)
            acc = jnp.dot(
                jnp.concatenate([picked[4 * HD :], ones_tail], 0),
                weights,
                preferred_element_type=F32,
            )
            total = acc[HD : HD + 1]
            own_out[item, 0:HD] = acc[0:HD] / total
            own_out[item, HD:88] = jnp.broadcast_to(top + jnp.log2(total), (8, ROWS))
            return carry

        lax.fori_loop(0, PLANE, one_block, 0, unroll=4)


def decode_choice(ids):
    lane = lax.broadcasted_iota(jnp.int32, (1, ROWS), 1)
    wanted = (lane % STEPS) * VOCAB + ids
    return (lax.broadcasted_iota(jnp.int32, (STEPS * VOCAB, ROWS), 0) == wanted).astype(BF16)


def fresh(where, own, recv, ids, dec, cosine, sine):
    return pl.pallas_call(
        fresh_kernel,
        out_shape=[
            jax.ShapeDtypeStruct((SLOTS, 256, TILE), BF16),
            jax.ShapeDtypeStruct((SLOTS, 1, TILE), F32),
            jax.ShapeDtypeStruct((SLOTS, 96, TILE), F32),
            jax.ShapeDtypeStruct((PLANE, 88, ROWS), F32),
        ],
        in_specs=[sm()] + [vm()] * 6,
        out_specs=[vm()] * 4,
        scratch_shapes=[
            pltpu.VMEM((8, TILE, 256), BF16),
            pltpu.VMEM((8, 96, TILE), BF16),
            pltpu.VMEM((5 * HD, STEPS * VOCAB), BF16),
        ],
        compiler_params=params(),
        name="fresh",
    )(where, own, recv, ids, dec, cosine, sine)


BLOCKS = PLANE * 3 + KB // 128 + 2


def cached_kernel(
    where_ref,
    length_ref,
    mine_ref,
    peer_ref,
    query_ref,
    max_in,
    acc_in,
    sent_ref,
    kept_ref,
    key_buf,
    value_buf,
    keys,
    values,
    max_ref,
    acc_ref,
    sems,
):
    group = where_ref[0]

    @pl.when(group == 0)
    def _():
        pltpu.make_async_copy(mine_ref, key_buf, sems.at[0]).start()
        pltpu.make_async_copy(peer_ref, value_buf, sems.at[1]).start()

    @pl.when(group != 0)
    def _():
        pltpu.make_async_copy(peer_ref, key_buf, sems.at[0]).start()
        pltpu.make_async_copy(mine_ref, value_buf, sems.at[1]).start()

    pltpu.make_async_copy(mine_ref, key_buf, sems.at[0]).wait()
    pltpu.make_async_copy(mine_ref, value_buf, sems.at[1]).wait()
    lane = lax.broadcasted_iota(jnp.int32, (16, CACHE), 1)
    row16 = lax.broadcasted_iota(jnp.int32, (16, CACHE), 0)
    ones_row = first_row((16, 128), 1.0).astype(BF16)

    def pack(source, count):
        length = length_ref[source]
        bias = jnp.where((row16 == 0) & (lane >= length), DEAD, 0.0).astype(BF16)
        part = key_buf[source]
        turned = jnp.concatenate([part, part, part, bias], 0).T
        for block in range(3):
            at = slice(block * 128, block * 128 + 128)
            keys[count + block] = turned[at]
            values[count + block] = jnp.concatenate([value_buf[source, :, at], ones_row], 0)
        return count + (length + 127) // 128

    count = lax.fori_loop(0, PLANE, pack, jnp.int32(0), unroll=2)
    dead_lane = lax.broadcasted_iota(jnp.int32, (128, 256), 1) == 3 * HD
    for block in range(KB // 128):
        keys[count + block] = jnp.where(dead_lane, DEAD, 0.0).astype(BF16)
        values[count + block] = jnp.zeros((96, 128), BF16)
    chunks = (count + KB // 128 - 1) // (KB // 128)

    for first in range(0, SLOTS, GS):
        here = jnp.where((first >= 8) & (group == 1), 0, chunks)
        for slot in range(first, first + GS):
            max_ref[slot] = max_in[slot]
            acc_ref[slot] = acc_in[slot]

        def chunk(step, carry, first=first):
            per = KB // 128
            key_part = jnp.concatenate([keys[per * step + block] for block in range(per)], 0)
            value_part = jnp.concatenate([values[per * step + block] for block in range(per)], 1)
            for slot in range(first, first + GS):
                max_ref[slot], acc_ref[slot] = flash_step(
                    query_ref[slot], key_part, value_part, max_ref[slot], acc_ref[slot]
                )
            return carry

        lax.fori_loop(0, here, chunk, 0)

        for slot in range(first, first + GS):
            acc = acc_ref[slot]
            total = jnp.where(here > 0, acc[HD : HD + 1], 1.0)
            pieces = split3(max_ref[slot] + jnp.log2(total))
            target, at = (sent_ref, slot) if slot < SENT else (kept_ref, slot - SENT)
            row = lax.broadcasted_iota(jnp.int32, (16, TILE), 0)
            tail = jnp.where(
                row == 0,
                pieces[0].astype(F32),
                jnp.where(row == 1, pieces[1].astype(F32), pieces[2].astype(F32)),
            )
            tail = jnp.where(row <= 2, tail, 0.0)
            target[at] = jnp.concatenate([acc[0:HD] / total, tail], 0).astype(BF16)


def cached(where, lengths, mine, peer, query, top, acc):
    return pl.pallas_call(
        cached_kernel,
        out_shape=[
            jax.ShapeDtypeStruct((SENT, 96, TILE), BF16),
            jax.ShapeDtypeStruct((SLOTS - SENT, 96, TILE), BF16),
        ],
        in_specs=[sm(), sm(), anyspace(), anyspace(), vm(), vm(), vm()],
        out_specs=[vm(), vm()],
        scratch_shapes=[
            pltpu.VMEM((PLANE, HD, CACHE), BF16),
            pltpu.VMEM((PLANE, HD, CACHE), BF16),
            pltpu.VMEM((BLOCKS, 128, 256), BF16),
            pltpu.VMEM((BLOCKS, 96, 128), BF16),
            pltpu.VMEM((SLOTS, 1, TILE), F32),
            pltpu.VMEM((SLOTS, 96, TILE), F32),
            pltpu.SemaphoreType.DMA((2,)),
        ],
        compiler_params=params(),
        name="cached",
    )(where, lengths, mine, peer, query, top, acc)


def spread_kernel(where_ref, sent_ref, kept_ref, got_ref, dec_ref, own_ref, out_ref):
    group = where_ref[0]
    plane = where_ref[1]

    @pl.when(group == 0)
    def _():
        for slot, tile in enumerate(TILES[0]):
            part = sent_ref[slot] if slot < SENT else kept_ref[slot - SENT]
            out_ref[2 * tile] = part[:, 0:ROWS]
            out_ref[2 * tile + 1] = part[:, ROWS:]
        for slot, tile in enumerate(TILES[1][:SENT]):
            part = got_ref[slot]
            out_ref[2 * tile] = part[:, 0:ROWS]
            out_ref[2 * tile + 1] = part[:, ROWS:]

    @pl.when(group == 1)
    def _():
        wide = jnp.concatenate([kept_ref[0], kept_ref[1]], 1)

        def pick(index):
            return jnp.dot(wide, decode_choice(dec_ref[index]), preferred_element_type=F32)

        def plain(item, carry):
            index = (1 - plane) * PLANE + item
            out_ref[index] = pick(index).astype(BF16)
            return carry

        lax.fori_loop(0, PLANE, plain, 0, unroll=2)

        def joined(item, carry):
            index = plane * PLANE + item
            picked = pick(index)
            here = picked[HD : HD + 1] + picked[HD + 1 : HD + 2] + picked[HD + 2 : HD + 3]
            own = own_ref[item]
            there = own[HD : HD + 1]
            top = jnp.maximum(here, there)
            left = jnp.exp2(here - top)
            right = jnp.exp2(there - top)
            total = left + right
            value = (picked[0:HD] * left + own[0:HD] * right) / total
            high, mid, low = split3(top + jnp.log2(total))
            row = lax.broadcasted_iota(jnp.int32, (16, ROWS), 0)
            tail = jnp.where(
                row == 0,
                high.astype(F32),
                jnp.where(row == 1, mid.astype(F32), low.astype(F32)),
            )
            tail = jnp.where(row <= 2, tail, 0.0)
            out_ref[index] = jnp.concatenate([value, tail], 0).astype(BF16)
            return carry

        lax.fori_loop(0, PLANE, joined, 0, unroll=2)


def spread(where, sent, kept, got, dec, own):
    return pl.pallas_call(
        spread_kernel,
        out_shape=jax.ShapeDtypeStruct((N_CTX, 96, ROWS), BF16),
        in_specs=[sm()] + [vm()] * 5,
        out_specs=vm(),
        compiler_params=params(),
        name="spread",
    )(where, sent, kept, got, dec, own)


def join_kernel(parts_ref, out_ref, wide):
    for head in range(PLANE):
        first = parts_ref[head].astype(F32)
        second = parts_ref[PLANE + head].astype(F32)
        one = first[HD : HD + 1] + first[HD + 1 : HD + 2] + first[HD + 2 : HD + 3]
        two = second[HD : HD + 1] + second[HD + 1 : HD + 2] + second[HD + 2 : HD + 3]
        top = jnp.maximum(one, two)
        left = jnp.exp2(one - top)
        right = jnp.exp2(two - top)
        total = left + right
        wide[head * HD : head * HD + HD, :] = (
            first[0:HD] * (left / total) + second[0:HD] * (right / total)
        )
    for block in range(HALF // 128):
        lanes = slice(block * 128, block * 128 + 128)
        out_ref[:, lanes] = wide[lanes, :].T.astype(BF16)


def join(parts):
    return pl.pallas_call(
        join_kernel,
        out_shape=jax.ShapeDtypeStruct((ROWS, HALF), BF16),
        in_specs=[vm()],
        out_specs=vm(),
        scratch_shapes=[pltpu.VMEM((HALF, ROWS), F32)],
        compiler_params=params(),
        name="join",
    )(parts)


def angle_tables(offset):
    quarter = HD // 4
    frequency = 10000.0 ** (-jnp.arange(quarter, dtype=F32) / quarter)
    lane = jnp.arange(TILE, dtype=jnp.int32)
    step = jnp.arange(STEPS, dtype=jnp.int32)
    base = offset // PROT
    column = jnp.concatenate([(offset + lane) % PROT, (offset + PLANE * TILE + step) % PROT])
    homolog = base + jnp.arange(20, dtype=jnp.int32)
    column_angle = frequency[:, None] * column.astype(F32)[None]
    homolog_angle = frequency[:, None] * homolog.astype(F32)[None]
    carry = (offset % PROT + lane) >= PROT
    step_homolog = (offset + PLANE * TILE + step) // PROT - base

    def tiles(function):
        columns = function(column_angle)
        homologs = function(homolog_angle)
        low = homologs[:, 0:16].T[:, :, None]
        high = homologs[:, 1:17].T[:, :, None]
        second = jnp.where(carry[None, None, :], high, low)
        first = jnp.broadcast_to(columns[None, :, :TILE], second.shape)
        whole = jnp.concatenate([first, first, second, second], 1)
        pick = (jnp.arange(20)[:, None] == step_homolog[None, :]).astype(F32)
        dec_second = jnp.sum(homologs[:, :, None] * pick[None], 1)
        dec_first = columns[:, TILE:]
        dec = jnp.concatenate([dec_first, dec_first, dec_second, dec_second], 0)
        dec = jnp.repeat(dec, VOCAB, axis=1).reshape(HD, 2, TILE).transpose(1, 0, 2)
        return jnp.concatenate([whole, dec], 0)

    return tiles(jnp.cos), tiles(jnp.sin)


def local(
    token_ids,
    span_offset,
    shard_lengths,
    embed_table,
    norm_gain,
    query_weight,
    key_weight,
    value_weight,
    cache_keys,
    cache_values,
):
    group = lax.axis_index("group")
    plane = lax.axis_index("yh")
    head = lax.axis_index("zx")
    mp = lax.axis_index("mp")
    tiles = jnp.where(group == 0, jnp.array(TILES[0], jnp.int32), jnp.array(TILES[1], jnp.int32))
    where = jnp.concatenate([jnp.stack([group, plane, mp, head]).astype(jnp.int32), tiles])
    swap = [(0, 1), (1, 0)]

    turned = turn(where, cache_keys, cache_values).reshape(PLANE, HD, CACHE)
    mine = lax.all_to_all(turned, "zx", 0, 0, tiled=True)
    peer = lax.ppermute(mine, "group", swap)

    small = jnp.concatenate([token_ids, jnp.broadcast_to(shard_lengths[None], (1, 128))], 0)
    small = jnp.broadcast_to(small[None], (N_CTX, 2, 128))
    small = lax.all_to_all(small, ("yh", "zx"), 0, 0, tiled=True)
    mine_ids = small[:, 0]
    lengths = lax.dynamic_slice(small[:, 1, 0], (plane * PLANE,), (PLANE,))
    prefill_ids = lax.ppermute(mine_ids, "group", [(0, 1)])
    prefill_ids = jnp.where(group == 0, mine_ids, prefill_ids)
    decode_ids = mine_ids.reshape(N_CTX, 1, ROWS)
    table_ids = jnp.broadcast_to(jnp.arange(TILE, dtype=jnp.int32) % VOCAB, (2, TILE))
    ids = jnp.concatenate([prefill_ids.reshape(PLANE, TILE), table_ids], 0)[:, None, :]

    wide_embed = embed_table.astype(F32)
    square = jnp.sum(wide_embed * wide_embed, 1)
    square = square + lax.ppermute(square, "mp", swap)
    own, other = table(
        where,
        embed_table,
        norm_gain[None],
        square[:, None],
        query_weight,
        key_weight,
        value_weight,
    )
    recv = lax.ppermute(other, "mp", swap)
    cosine, sine = angle_tables(span_offset[0])
    query, top, acc, own_part = fresh(where, own, recv, ids, decode_ids, cosine, sine)
    sent, kept = cached(where, lengths, mine, peer, query, top, acc)
    got = lax.ppermute(sent, "group", [(1, 0)])
    blocks = spread(where, sent, kept, got, decode_ids, own_part)
    parts = lax.all_to_all(blocks, ("yh", "zx"), 0, 0, tiled=True)
    return join(parts)[None]


def solution(mesh):
    inner = Mesh(mesh.devices.reshape(2, 2, PLANE, 2), ("group", "yh", "zx", "mp"))
    ctx = ("yh", "zx")
    placed = (
        P("group", ctx),
        P(),
        P(ctx),
        P(None, "mp"),
        P("mp"),
        P("mp", None),
        P("mp", None),
        P("mp", None),
        P(ctx, "mp"),
        P(ctx, "mp"),
    )
    return jax.shard_map(
        local, mesh=inner, in_specs=placed, out_specs=P("group", ctx, "mp"), check_vma=False
    )
```

```python
import math

import jax
import jax.numpy as jnp
from jax import lax
from jax.experimental import pallas as pl
from jax.experimental.pallas import tpu as pltpu
from jax.sharding import Mesh
from jax.sharding import PartitionSpec as P

D = 2560
HALF = 1280
HD = 80
PROT = 256
STEPS = 4
VOCAB = 128
PLANE = 16
N_CTX = 32
ROWS = 128
CACHE = 384
CHUNK = 88
TILE = 256
SLOTS = 10
SENT = 6
KB = 1024
GROUPS = ((0, 4), (4, 8), (8, 10))
FAR = 96.0
SCALE2 = math.log2(math.e) / math.sqrt(HD)
LOW = -1e30
DEAD = -2e30
F32 = jnp.float32
BF16 = jnp.bfloat16
TILES = ((0, 1, 2, 3, 10, 11, 12, 13, 14, 15), (4, 5, 6, 7, 8, 9, 16, 17, 0, 0))


def vm():
    return pl.BlockSpec(memory_space=pltpu.MemorySpace.VMEM)


def sm():
    return pl.BlockSpec(memory_space=pltpu.MemorySpace.SMEM)


def anyspace():
    return pl.BlockSpec(memory_space=pl.ANY)


def far():
    return pl.BlockSpec(memory_space=pltpu.MemorySpace.HBM)


def params(mib):
    return pltpu.CompilerParams(vmem_limit_bytes=mib << 20)


def split3(x):
    high = x.astype(BF16)
    rest = x - high.astype(F32)
    mid = rest.astype(BF16)
    low = (rest - mid.astype(F32)).astype(BF16)
    return high, mid, low


def first_row(shape, value):
    return jnp.where(lax.broadcasted_iota(jnp.int32, shape, 0) == 0, value, 0.0)


def turn_kernel(where_ref, small_ref, keys_ref, values_ref, out_ref, buf, sem):
    @pl.when(where_ref[0] == 0)
    def _():
        pltpu.make_async_copy(keys_ref, buf, sem).start()

    @pl.when(where_ref[0] != 0)
    def _():
        pltpu.make_async_copy(values_ref, buf, sem).start()

    small = small_ref[...].astype(BF16)
    for head in range(PLANE):
        out_ref[head, HD:] = small
    pltpu.make_async_copy(keys_ref, buf, sem).wait()
    for block in range(HALF // 128):
        part = buf[:, block * 128 : block * 128 + 128].T
        row = block * 128
        while row < block * 128 + 128:
            head = row // HD
            end = min((head + 1) * HD, block * 128 + 128)
            out_ref[head, row - head * HD : end - head * HD] = part[
                row - block * 128 : end - block * 128
            ]
            row = end


def turn(where, small, keys, values):
    return pl.pallas_call(
        turn_kernel,
        out_shape=jax.ShapeDtypeStruct((PLANE, CHUNK, CACHE), BF16),
        in_specs=[sm(), vm(), far(), far()],
        out_specs=vm(),
        scratch_shapes=[pltpu.VMEM((CACHE, HALF), BF16), pltpu.SemaphoreType.DMA(())],
        compiler_params=params(56),
        name="turn",
    )(where, small, keys, values)


def gate_kernel(value_ref, earlier_ref, out_ref):
    del value_ref, earlier_ref, out_ref


def gate(value, earlier):
    return pl.pallas_call(
        gate_kernel,
        out_shape=jax.ShapeDtypeStruct(value.shape, value.dtype),
        in_specs=[anyspace(), anyspace()],
        out_specs=anyspace(),
        input_output_aliases={0: 0},
        name="gate",
    )(value, earlier)


def table_kernel(where_ref, embed_ref, gain_ref, square_ref, wq, wk, wv, own_ref, other_ref, buf, turned, sems):
    mp = where_ref[2]
    head = where_ref[3]
    base = jnp.minimum((head * HD) // 128 * 128, 1024)
    inside = pl.multiple_of(head * HD - base, 16)
    halves = (mp, 1 - mp)
    for half in range(2):
        at = pl.multiple_of(halves[half] * HALF + base, 128)
        for which, weight in enumerate((wq, wk, wv)):
            pltpu.make_async_copy(
                weight.at[:, pl.ds(at, 256)], buf.at[half * 3 + which], sems.at[half * 3 + which]
            ).start()
    mean = square_ref[...] / D
    normal = (
        embed_ref[...].astype(F32) * lax.rsqrt(mean + 1e-05) * gain_ref[...].astype(F32)
    ).astype(BF16)
    for half in (1, 0):
        for which in range(3):
            pltpu.make_async_copy(
                wq.at[:, pl.ds(0, 256)], buf.at[half * 3 + which], sems.at[half * 3 + which]
            ).wait()
            turned[...] = jnp.dot(normal, buf[half * 3 + which], preferred_element_type=F32).T
            out = own_ref if half == 0 else other_ref
            out[which * HD : which * HD + HD, :] = turned[pl.ds(inside, HD), :]


def table(where, embed, gain, square, wq, wk, wv):
    return pl.pallas_call(
        table_kernel,
        out_shape=[jax.ShapeDtypeStruct((3 * HD, VOCAB), F32)] * 2,
        in_specs=[sm(), vm(), vm(), vm(), far(), far(), far()],
        out_specs=[vm(), vm()],
        scratch_shapes=[
            pltpu.VMEM((6, HALF, 256), BF16),
            pltpu.VMEM((256, VOCAB), F32),
            pltpu.SemaphoreType.DMA((6,)),
        ],
        compiler_params=params(56),
        name="table",
    )(where, embed, gain, square, wq, wk, wv)


def fresh_kernel(
    where_ref,
    own_ref,
    recv_ref,
    mine_ref,
    column_ref,
    homolog_ref,
    step_ref,
    query_ref,
    max_ref,
    acc_ref,
    own_out,
    dec_ref,
    length_out,
    keys,
    values,
    wide,
    worst_ref,
    ids_ref,
):
    group = where_ref[0]
    plane = where_ref[1]
    quarter = HD // 4
    smalls = [mine_ref[source, HD:CHUNK, :].astype(F32) for source in range(PLANE)]
    sixteen = lax.broadcasted_iota(jnp.int32, (PLANE, 128), 0)
    length = jnp.zeros((PLANE, 128), F32)
    for source in range(PLANE):
        small = smalls[source]
        size = small[2:3, 0:128] * 16.0 + small[2:3, 128:256]
        length = jnp.where(sixteen == source, jnp.broadcast_to(size, (PLANE, 128)), length)
        for half in range(2):
            same = plane == half
            block = half * PLANE + source
            first = jnp.where(same, small[0:1, 0:128], small[0:1, 128:256])
            lanes = slice(source % 2 * ROWS, source % 2 * ROWS + ROWS)
            ids_ref[block // 2, :, lanes] = first.astype(jnp.int32)
            second = jnp.where(same, small[1:2, 0:128], small[1:2, 128:256])
            dec_ref[block] = second.astype(jnp.int32)
    length_out[...] = length.astype(jnp.int32)
    for part in range(2):
        ids_ref[PLANE + part] = lax.broadcasted_iota(jnp.int32, (1, TILE), 1) % VOCAB
    tables = own_ref[...] + recv_ref[...]
    row = lax.broadcasted_iota(jnp.int32, (HD, VOCAB), 0)
    upper = (row // quarter) % 2 == 0

    def stacked(part):
        partner = jnp.where(
            upper, -pltpu.roll(part, HD - quarter, 0), pltpu.roll(part, quarter, 0)
        )
        pieces = []
        for item in (part, partner):
            high = item.astype(BF16)
            pieces += [high, (item - high.astype(F32)).astype(BF16)]
        return jnp.concatenate(pieces, 0)

    query_table = stacked(tables[0:HD])
    key_table = stacked(tables[HD : 2 * HD])
    value_table = tables[2 * HD :].astype(BF16)
    tail_keys = jnp.zeros((16, TILE), BF16)
    ones_row = first_row((16, TILE), 1.0).astype(BF16)
    lane = lax.broadcasted_iota(jnp.int32, (1, TILE), 1)
    carried = lane + where_ref[14] >= PROT

    def chosen(tile):
        return (
            lax.broadcasted_iota(jnp.int32, (VOCAB, TILE), 0) == ids_ref[tile]
        ).astype(BF16)

    def homolog_at(which, tile):
        low = homolog_ref[which, tile]
        high = homolog_ref[which, tile + 1]
        return jnp.where(
            carried, jnp.concatenate([high, high], 1), jnp.concatenate([low, low], 1)
        )

    def turned_by(one_hot, stack, tile, decode=None):
        raw = jnp.dot(stack, one_hot, preferred_element_type=F32)
        plain = raw[0:HD] + raw[HD : 2 * HD]
        partner = raw[2 * HD : 3 * HD] + raw[3 * HD :]
        if decode is not None:
            return (plain * step_ref[0, decode] + partner * step_ref[1, decode]).astype(BF16)
        half = HD // 2
        first = plain[:half] * column_ref[0] + partner[:half] * column_ref[1]
        second = plain[half:] * homolog_at(0, tile) + partner[half:] * homolog_at(1, tile)
        return jnp.concatenate([first, second], 0).astype(BF16)

    def tile_of(slot):
        return where_ref[4 + slot]

    def put_query(slot, rotated):
        query_ref[slot] = jnp.concatenate([*split3(rotated.astype(F32) * SCALE2), ones_row], 0)

    def one_query(slot, carry):
        tile = tile_of(slot)
        put_query(slot, turned_by(chosen(tile), query_table, tile))
        return carry

    lax.fori_loop(0, jnp.where(group == 0, SLOTS, SENT), one_query, 0)

    def one_key(block, carry):
        tile = 2 * block + plane
        one_hot = chosen(tile)
        rotated = turned_by(one_hot, key_table, tile)
        keys[block] = jnp.concatenate([rotated, rotated, rotated, tail_keys], 0).T
        picked = jnp.dot(value_table, one_hot, preferred_element_type=F32).astype(BF16)
        values[block] = jnp.concatenate([picked, ones_row], 0)
        return carry

    lax.fori_loop(0, 8, one_key, 0, unroll=2)

    @pl.when(group == 1)
    def _():
        for part in range(2):
            lanes = slice(part * TILE, part * TILE + TILE)
            one_hot = chosen(16 + part)
            put_query(SENT + part, turned_by(one_hot, query_table, 0, part))
            query_ref[SENT + 2 + part] = jnp.zeros((256, TILE), BF16)
            wide[0 : 3 * HD, lanes] = query_ref[SENT + part, 0 : 3 * HD, :]
            wide[3 * HD : 4 * HD, lanes] = turned_by(one_hot, key_table, 0, part)
            wide[4 * HD : 5 * HD, lanes] = jnp.dot(
                value_table, one_hot, preferred_element_type=F32
            ).astype(BF16)


    def last_half(slot, half, state):
        tile = tile_of(slot)
        limit = jnp.where(tile >= PLANE, 1 << 20, tile * TILE) + lane
        top, acc = state
        scores = []
        for unit in range(4):
            block = 4 * half + unit
            part = jnp.dot(keys[block], query_ref[slot], preferred_element_type=F32)
            row_at = lax.broadcasted_iota(jnp.int32, (TILE, TILE), 0)
            seen = row_at + (2 * block + plane) * TILE <= limit
            scores.append(jnp.where(seen, part, DEAD))
        new = top
        for part in scores:
            new = jnp.maximum(new, jnp.max(part, 0, keepdims=True))
        total = None
        for unit in range(4):
            weights = jnp.exp2(scores[unit] - new).astype(BF16)
            piece = jnp.dot(values[4 * half + unit], weights, preferred_element_type=F32)
            total = piece if total is None else total + piece
        if acc is None:
            return new, total
        return new, acc * jnp.exp2(top - new) + total

    low_start = jnp.full((1, TILE), LOW, F32)

    def early(pair, carry):
        for slot in (2 * pair, 2 * pair + 1):
            max_ref[slot], acc_ref[slot] = last_half(slot, 0, (low_start, None))
        return carry

    lax.fori_loop(0, 2, early, 0)
    worst_ref[...] = jnp.zeros((1, TILE), F32)

    def late(pair, carry):
        for slot in (2 * pair, 2 * pair + 1):
            top, acc = last_half(slot, 1, (low_start, None))
            first = jnp.dot(keys[0], query_ref[slot], preferred_element_type=F32)
            base = jnp.maximum(top, jnp.max(first, 0, keepdims=True))
            new, total, peak = stale_units(
                [(keys[unit], values[unit]) for unit in range(4)], query_ref[slot], base
            )
            worst_ref[...] = jnp.maximum(worst_ref[...], peak - base)
            acc = acc * jnp.exp2(top - base) + total
            max_ref[slot] = new
            acc_ref[slot] = acc * jnp.exp2(base - new)
        return carry

    pairs = jnp.where(group == 0, SLOTS // 2, SLOTS // 2 - 1)
    lax.fori_loop(2, pairs, late, 0)

    @pl.when(jnp.max(worst_ref[...]) > FAR)
    def _():
        def again(slot, carry):
            state = last_half(slot, 1, (low_start, None))
            max_ref[slot], acc_ref[slot] = last_half(slot, 0, state)
            return carry

        lax.fori_loop(4, 2 * pairs, again, 0)

    @pl.when(group == 1)
    def _():
        key_at = lax.broadcasted_iota(jnp.int32, (TILE, TILE), 0)
        query_at = lax.broadcasted_iota(jnp.int32, (TILE, TILE), 1)
        seen = (key_at // STEPS == query_at // STEPS) & (key_at <= query_at)

        def one_block(item, carry):
            at = plane * PLANE + 2 * item
            one_hot = decode_choice(jnp.concatenate([dec_ref[at], dec_ref[at + 1]], 1))
            picked = jnp.dot(wide[...], one_hot, preferred_element_type=F32).astype(BF16)
            queries = jnp.concatenate([picked[0 : 3 * HD], ones_row], 0)
            own_keys = picked[3 * HD : 4 * HD]
            own_keys = jnp.concatenate([own_keys, own_keys, own_keys, tail_keys], 0).T
            scores = jnp.dot(own_keys, queries, preferred_element_type=F32)
            scores = jnp.where(seen, scores, DEAD)
            top = jnp.max(scores, 0, keepdims=True)
            weights = jnp.exp2(scores - top).astype(BF16)
            acc = jnp.dot(
                jnp.concatenate([picked[4 * HD :], ones_row], 0),
                weights,
                preferred_element_type=F32,
            )
            total = acc[HD : HD + 1]
            value = acc[0:HD] / total
            log_sum = jnp.broadcast_to(top + jnp.log2(total), (8, TILE))
            for part in range(2):
                lanes = slice(part * ROWS, part * ROWS + ROWS)
                own_out[2 * item + part, 0:HD] = value[:, lanes]
                own_out[2 * item + part, HD:88] = log_sum[:, lanes]
            return carry

        lax.fori_loop(0, PLANE // 2, one_block, 0, unroll=2)


def stale_units(units, query, base):
    peak = base
    total = None
    for key_part, value_part in units:
        scores = jnp.dot(key_part, query, preferred_element_type=F32)
        weights = jnp.exp2(scores - base).astype(BF16)
        peak = jnp.maximum(peak, jnp.max(scores, 0, keepdims=True))
        piece = jnp.dot(value_part, weights, preferred_element_type=F32)
        total = piece if total is None else total + piece
    return peak, total, peak


def decode_choice(ids):
    lane = lax.broadcasted_iota(jnp.int32, ids.shape, 1)
    wanted = (lane % STEPS) * VOCAB + ids
    rows = lax.broadcasted_iota(jnp.int32, (STEPS * VOCAB, ids.shape[1]), 0)
    return (rows == wanted).astype(BF16)


def fresh(where, own, recv, mine, column, homolog, step):
    return pl.pallas_call(
        fresh_kernel,
        out_shape=[
            jax.ShapeDtypeStruct((SLOTS, 256, TILE), BF16),
            jax.ShapeDtypeStruct((SLOTS, 1, TILE), F32),
            jax.ShapeDtypeStruct((SLOTS, 96, TILE), F32),
            jax.ShapeDtypeStruct((PLANE, 88, ROWS), F32),
            jax.ShapeDtypeStruct((N_CTX, 1, ROWS), jnp.int32),
            jax.ShapeDtypeStruct((PLANE, 128), jnp.int32),
        ],
        in_specs=[sm()] + [vm()] * 6,
        out_specs=[vm()] * 6,
        scratch_shapes=[
            pltpu.VMEM((8, TILE, 256), BF16),
            pltpu.VMEM((8, 96, TILE), BF16),
            pltpu.VMEM((5 * HD, STEPS * VOCAB), BF16),
            pltpu.VMEM((1, TILE), F32),
            pltpu.VMEM((PLANE + 2, 1, TILE), jnp.int32),
        ],
        compiler_params=params(20),
        name="fresh",
    )(where, own, recv, mine, column, homolog, step)


BLOCKS = PLANE * 3 + KB // 128 + 2


def cached_kernel(
    where_ref,
    length_ref,
    mine_ref,
    peer_ref,
    query_ref,
    max_in,
    acc_in,
    sent_ref,
    kept_ref,
    key_buf,
    value_buf,
    keys,
    values,
    max_ref,
    acc_ref,
    worst_ref,
    sems,
):
    group = where_ref[0]

    @pl.when(group == 0)
    def _():
        pltpu.make_async_copy(mine_ref, key_buf, sems.at[0]).start()
        pltpu.make_async_copy(peer_ref, value_buf, sems.at[1]).start()

    @pl.when(group != 0)
    def _():
        pltpu.make_async_copy(peer_ref, key_buf, sems.at[0]).start()
        pltpu.make_async_copy(mine_ref, value_buf, sems.at[1]).start()

    pltpu.make_async_copy(mine_ref, key_buf, sems.at[0]).wait()
    pltpu.make_async_copy(mine_ref, value_buf, sems.at[1]).wait()
    lane = lax.broadcasted_iota(jnp.int32, (16, CACHE), 1)
    row16 = lax.broadcasted_iota(jnp.int32, (16, CACHE), 0)
    ones_row = first_row((16, 128), 1.0).astype(BF16)

    def pack(source, count):
        length = length_ref[source, 0]
        bias = jnp.where((row16 == 0) & (lane >= length), DEAD, 0.0).astype(BF16)
        part = key_buf[source, 0:HD]
        turned = jnp.concatenate([part, part, part, bias], 0).T
        for block in range(3):
            at = slice(block * 128, block * 128 + 128)
            keys[count + block] = turned[at]
            values[count + block] = jnp.concatenate([value_buf[source, 0:HD, at], ones_row], 0)
        return count + (length + 127) // 128

    count = lax.fori_loop(0, PLANE, pack, jnp.int32(0), unroll=2)
    dead_lane = lax.broadcasted_iota(jnp.int32, (128, 256), 1) == 3 * HD
    for block in range(KB // 128):
        keys[count + block] = jnp.where(dead_lane, DEAD, 0.0).astype(BF16)
        values[count + block] = jnp.zeros((96, 128), BF16)
    chunks = (count + KB // 128 - 1) // (KB // 128)

    per = KB // 128
    starter = jnp.concatenate([keys[0], keys[1]], 0)
    worst_ref[...] = jnp.zeros((1, TILE), F32)

    def chunk_units(step):
        units = []
        for unit in range(per // 2):
            at = per * step + 2 * unit
            units.append(
                (
                    jnp.concatenate([keys[at], keys[at + 1]], 0),
                    jnp.concatenate([values[at], values[at + 1]], 1),
                )
            )
        return units

    for first, end in GROUPS:
        here = jnp.where((first >= 8) & (group == 1), 0, chunks)
        for slot in range(first, end):
            peak = jnp.max(
                jnp.dot(starter, query_ref[slot], preferred_element_type=F32), 0, keepdims=True
            )
            top = jnp.maximum(max_in[slot], peak)
            max_ref[slot] = top
            acc_ref[slot] = acc_in[slot] * jnp.exp2(max_in[slot] - top)

        def chunk(step, carry, first=first, end=end):
            units = chunk_units(step)
            for slot in range(first, end):
                base = max_ref[slot]
                new, total, peak = stale_units(units, query_ref[slot], base)
                worst_ref[...] = jnp.maximum(worst_ref[...], peak - base)
                max_ref[slot] = new
                acc_ref[slot] = (acc_ref[slot] + total) * jnp.exp2(base - new)
            return carry

        lax.fori_loop(0, here, chunk, 0)

    slots = jnp.where(group == 0, SLOTS, SLOTS - 2)

    @pl.when(jnp.max(worst_ref[...]) > FAR)
    def _():
        def one_slot(slot, carry):
            max_ref[slot] = max_in[slot]
            acc_ref[slot] = acc_in[slot]

            def one_chunk(block, inner):
                top = max_ref[slot]
                scores = jnp.dot(keys[block], query_ref[slot], preferred_element_type=F32)
                new = jnp.maximum(top, jnp.max(scores, 0, keepdims=True))
                weights = jnp.exp2(scores - new).astype(BF16)
                max_ref[slot] = new
                acc_ref[slot] = acc_ref[slot] * jnp.exp2(top - new) + jnp.dot(
                    values[block], weights, preferred_element_type=F32
                )
                return inner

            lax.fori_loop(0, count, one_chunk, 0)
            return carry

        lax.fori_loop(0, slots, one_slot, 0)

    row = lax.broadcasted_iota(jnp.int32, (16, TILE), 0)
    for slot in range(SLOTS):
        acc = acc_ref[slot]
        total = jnp.where(slot < slots, acc[HD : HD + 1], 1.0)
        high, mid, low = split3(max_ref[slot] + jnp.log2(total))
        target, at = (sent_ref, slot) if slot < SENT else (kept_ref, slot - SENT)
        tail = jnp.where(
            row == 0,
            high.astype(F32),
            jnp.where(row == 1, mid.astype(F32), low.astype(F32)),
        )
        tail = jnp.where(row <= 2, tail, 0.0)
        target[at] = jnp.concatenate([acc[0:HD] * (1.0 / total), tail], 0).astype(BF16)


def cached(where, lengths, mine, peer, query, top, acc):
    return pl.pallas_call(
        cached_kernel,
        out_shape=[
            jax.ShapeDtypeStruct((SENT, 96, TILE), BF16),
            jax.ShapeDtypeStruct((SLOTS - SENT, 96, TILE), BF16),
        ],
        in_specs=[sm(), sm(), anyspace(), anyspace(), vm(), vm(), vm()],
        out_specs=[vm(), vm()],
        scratch_shapes=[
            pltpu.VMEM((PLANE, CHUNK, CACHE), BF16),
            pltpu.VMEM((PLANE, CHUNK, CACHE), BF16),
            pltpu.VMEM((BLOCKS, 128, 256), BF16),
            pltpu.VMEM((BLOCKS, 96, 128), BF16),
            pltpu.VMEM((SLOTS, 1, TILE), F32),
            pltpu.VMEM((SLOTS, 96, TILE), F32),
            pltpu.VMEM((1, TILE), F32),
            pltpu.SemaphoreType.DMA((2,)),
        ],
        compiler_params=params(24),
        name="cached",
    )(where, lengths, mine, peer, query, top, acc)


def spread_kernel(where_ref, sent_ref, kept_ref, got_ref, dec_ref, own_ref, out_ref):
    group = where_ref[0]
    plane = where_ref[1]

    @pl.when(group == 0)
    def _():
        for slot, tile in enumerate(TILES[0]):
            part = sent_ref[slot] if slot < SENT else kept_ref[slot - SENT]
            out_ref[2 * tile] = part[:, 0:ROWS]
            out_ref[2 * tile + 1] = part[:, ROWS:]
        for slot, tile in enumerate(TILES[1][:SENT]):
            part = got_ref[slot]
            out_ref[2 * tile] = part[:, 0:ROWS]
            out_ref[2 * tile + 1] = part[:, ROWS:]

    @pl.when(group == 1)
    def _():
        wide = jnp.concatenate([kept_ref[0], kept_ref[1]], 1)

        def pick(index):
            ids = jnp.concatenate([dec_ref[index], dec_ref[index + 1]], 1)
            return jnp.dot(wide, decode_choice(ids), preferred_element_type=F32)

        def put(index, value):
            value = value.astype(BF16)
            out_ref[index] = value[:, 0:ROWS]
            out_ref[index + 1] = value[:, ROWS:]

        row = lax.broadcasted_iota(jnp.int32, (16, TILE), 0)

        def pair(item, carry):
            index = (1 - plane) * PLANE + 2 * item
            put(index, pick(index))
            index = plane * PLANE + 2 * item
            picked = pick(index)
            here = picked[HD : HD + 1] + picked[HD + 1 : HD + 2] + picked[HD + 2 : HD + 3]
            own = jnp.concatenate([own_ref[2 * item], own_ref[2 * item + 1]], 1)
            there = own[HD : HD + 1]
            top = jnp.maximum(here, there)
            left = jnp.exp2(here - top)
            right = jnp.exp2(there - top)
            total = left + right
            value = picked[0:HD] * (left / total) + own[0:HD] * (right / total)
            high, mid, low = split3(top + jnp.log2(total))
            tail = jnp.where(
                row == 0,
                high.astype(F32),
                jnp.where(row == 1, mid.astype(F32), low.astype(F32)),
            )
            tail = jnp.where(row <= 2, tail, 0.0)
            put(index, jnp.concatenate([value, tail], 0))
            return carry

        lax.fori_loop(0, PLANE // 2, pair, 0, unroll=2)


def spread(where, sent, kept, got, dec, own):
    return pl.pallas_call(
        spread_kernel,
        out_shape=jax.ShapeDtypeStruct((N_CTX, 96, ROWS), BF16),
        in_specs=[sm()] + [vm()] * 5,
        out_specs=vm(),
        compiler_params=params(12),
        name="spread",
    )(where, sent, kept, got, dec, own)


def join_kernel(parts_ref, out_ref, wide):
    for head in range(PLANE):
        first = parts_ref[head].astype(F32)
        second = parts_ref[PLANE + head].astype(F32)
        one = first[HD : HD + 1] + first[HD + 1 : HD + 2] + first[HD + 2 : HD + 3]
        two = second[HD : HD + 1] + second[HD + 1 : HD + 2] + second[HD + 2 : HD + 3]
        top = jnp.maximum(one, two)
        left = jnp.exp2(one - top)
        right = jnp.exp2(two - top)
        total = left + right
        wide[head * HD : head * HD + HD, :] = (
            first[0:HD] * (left / total) + second[0:HD] * (right / total)
        )
    for block in range(HALF // 128):
        lanes = slice(block * 128, block * 128 + 128)
        out_ref[:, lanes] = wide[lanes, :].T.astype(BF16)


def join(parts):
    return pl.pallas_call(
        join_kernel,
        out_shape=jax.ShapeDtypeStruct((ROWS, HALF), BF16),
        in_specs=[vm()],
        out_specs=vm(),
        scratch_shapes=[pltpu.VMEM((HALF, ROWS), F32)],
        compiler_params=params(8),
        name="join",
    )(parts)


def angle_tables(offset):
    quarter = HD // 4
    frequency = 10000.0 ** (-jnp.arange(quarter, dtype=F32) / quarter)
    lane = jnp.arange(TILE, dtype=jnp.int32)
    step = offset + PLANE * TILE + jnp.arange(STEPS, dtype=jnp.int32)
    homolog = offset // PROT + jnp.arange(PLANE + 1, dtype=jnp.int32)
    parts = [(offset + lane) % PROT, homolog, step % PROT, step // PROT]
    values = jnp.concatenate(parts).astype(F32)
    angle = jnp.tile(frequency, 2)[:, None] * values[None]
    both = jnp.stack([jnp.cos(angle), jnp.sin(angle)])
    column = both[:, :, :TILE]
    end = TILE + PLANE + 1
    homologs = both[:, :, TILE:end].transpose(0, 2, 1)
    homologs = jnp.broadcast_to(homologs[..., None], (2, PLANE + 1, HD // 2, 128))
    steps = jnp.concatenate([both[:, :, end : end + 4], both[:, :, end + 4 :]], 1)
    steps = steps.transpose(0, 2, 1).reshape(2, 2, 2, HD, 1)
    steps = jnp.broadcast_to(steps, (2, 2, 2, HD, VOCAB)).transpose(0, 1, 3, 2, 4)
    return column, homologs, steps.reshape(2, 2, HD, TILE)


def local(
    token_ids,
    span_offset,
    shard_lengths,
    embed_table,
    norm_gain,
    query_weight,
    key_weight,
    value_weight,
    cache_keys,
    cache_values,
):
    group = lax.axis_index("group")
    plane = lax.axis_index("yh")
    head = lax.axis_index("zx")
    mp = lax.axis_index("mp")
    tiles = jnp.where(group == 0, jnp.array(TILES[0], jnp.int32), jnp.array(TILES[1], jnp.int32))
    inside = span_offset % PROT
    where = jnp.concatenate([jnp.stack([group, plane, mp, head]).astype(jnp.int32), tiles, inside])
    swap = [(0, 1), (1, 0)]

    row = token_ids.astype(F32)
    beside = lax.ppermute(row, "yh", swap)
    upper = lax.ppermute(row, "group", [(0, 1)])
    across = lax.ppermute(row, ("group", "yh"), [(0, 3), (1, 2)])
    first = jnp.concatenate([row, beside], 1)
    prefill = jnp.where(group == 0, first, jnp.concatenate([upper, across], 1))
    size = jnp.broadcast_to(shard_lengths[None], (1, 128))
    sizes = jnp.concatenate([size // 16, size % 16], 1).astype(F32)
    small = jnp.pad(jnp.concatenate([prefill, first, sizes], 0), ((0, 5), (0, 128)))
    mine = lax.all_to_all(turn(where, small, cache_keys, cache_values), "zx", 0, 0, tiled=True)

    wide_embed = embed_table.astype(F32)
    square = jnp.sum(wide_embed * wide_embed, 1)
    square = square + lax.ppermute(square, "mp", swap)
    own, other = table(
        where,
        embed_table,
        norm_gain[None],
        square[:, None],
        query_weight,
        key_weight,
        value_weight,
    )
    recv = lax.ppermute(other, "mp", swap)
    mine = gate(mine, recv)
    peer = lax.ppermute(mine, "group", swap)
    angles = angle_tables(span_offset[0])
    query, top, acc, own_part, dec, lengths = fresh(where, own, recv, mine, *angles)
    sent, kept = cached(where, lengths, mine, peer, query, top, acc)
    got = lax.ppermute(sent, "group", [(1, 0)])
    blocks = spread(where, sent, kept, got, dec, own_part)
    parts = lax.all_to_all(blocks, ("yh", "zx"), 0, 0, tiled=True)
    return join(parts)[None]


def solution(mesh):
    inner = Mesh(mesh.devices.reshape(2, 2, PLANE, 2), ("group", "yh", "zx", "mp"))
    ctx = ("yh", "zx")
    placed = (
        P("group", ctx),
        P(),
        P(ctx),
        P(None, "mp"),
        P("mp"),
        P("mp", None),
        P("mp", None),
        P("mp", None),
        P(ctx, "mp"),
        P(ctx, "mp"),
    )
    return jax.shard_map(
        local, mesh=inner, in_specs=placed, out_specs=P("group", ctx, "mp"), check_vma=False
    )
```
